32 devices in a mesh: groups: 2 (over y), px: 16 (over z, x, core).
Axes of the slice: x: 2, y: 2, z: 4, core: 2. Of those that a mesh axis runs over, the one named last changes fastest.
Arguments:
- features: bfloat16 [32, 256, 256, 256], P(None, ('groups', 'px')), parts along dimension 1, may hold values from -6 to 6
- pointwise_weight: bfloat16 [32, 32], replicated, may hold values from -1 to 1
- pointwise_bias: float32 [32], replicated, may hold values from -3 to 3
- spectral_weight: float32 [2, 32, 32, 16384], P(None, None, None, 'px'), may hold values from -6 to 6
Outputs:
- updated: bfloat16 [32, 256, 256, 256], P(None, ('groups', 'px')), parts along dimension 1
The draws below stay inside these ranges and needn't reach their ends.
There are 2 independent parts, one for each index of `groups`. The reference program is written for one: setup_inputs(seed, part) draws one part's arguments, and reference() takes and returns one part's arrays. A program takes and returns all parts, laid end to end along the dimension named above; an argument that names none is the same for every part. Nothing has to cross between parts.
All inputs are finite; a program needn't handle non-finite values.
Results may differ from the reference program's by a relative error of at most 0.0025.
Values sent between devices are 32-bit elements; how exact they have to be, the bound alone decides.
No kernel may reach another device: no remote copies, remote signals or barrier semaphores. Data moves between devices by JAX's collectives and lax.ppermute only.
A program may use at most 256 MiB of HBM per device.

```python
import math
import jax
import jax.numpy as jnp
from jax import lax

C = 32
X = 128
Y = 256
Z = 256
KX = 32
KY = 32
KZ = 16
MODES = 16384


def steps_of(key, shape, cuts, least, largest):
    level = 1.0
    for axis_at, parts in cuts:
        draws = jax.random.uniform(jax.random.fold_in(jax.random.fold_in(key, 6), axis_at), (parts,), jnp.float32, least / len(cuts), largest / len(cuts))
        level = level * jnp.repeat(jnp.exp(draws), shape[axis_at] // parts).reshape((-1,) + (1,) * (len(shape) - 1 - axis_at))
    return level


def gaussian(key, dims, scale, most, cuts=(), kind=jnp.bfloat16):
    drawn = scale * jax.random.normal(key, dims, jnp.float32)
    if cuts:
        drawn = drawn * steps_of(key, dims, cuts, -0.22, 0.18)
    return jnp.clip(drawn, -most, most).astype(kind)


def setup_inputs(seed: int = 0, part: int = 0) -> dict:
    seeds = jax.random.split(jax.random.key(seed), 5)
    own_keys = jax.random.split(jax.random.fold_in(seeds[4], part), 5)
    features = gaussian(own_keys[0], (C, X, Y, Z), 1.0, 6.0, ((1, 16),))
    pointwise_weight = gaussian(seeds[1], (C, C), C ** -0.5, 1.0)
    pointwise_bias = gaussian(seeds[2], (C,), 0.5, 3.0, (), jnp.float32)
    spectral_weight = gaussian(seeds[3], (2, C, C, MODES), 1.0, 6.0, ((3, 16),), jnp.float32)
    return {"features": features, "pointwise_weight": pointwise_weight, "pointwise_bias": pointwise_bias, "spectral_weight": spectral_weight}


TWO_PI = 2.0 * math.pi


def signed_modes(number):
    ladder = jnp.arange(number, dtype=jnp.int32)
    return jnp.where(ladder < number // 2, ladder, ladder - number)


def phase_table(positions, frequency, length):
    product = (positions[:, None] * frequency[None, :]) % length
    return product.astype(jnp.float32) * (TWO_PI / length)


def forward_table(positions):
    x_phase = phase_table(positions, signed_modes(KX), X)
    cosine = jnp.cos(x_phase)
    sine = jnp.sin(x_phase)
    return jnp.stack([jnp.stack([cosine, -sine], axis=1), jnp.stack([sine, cosine], axis=1)], axis=0)


def inverse_table(positions):
    x_phase = phase_table(positions, signed_modes(KX), X)
    cosine = jnp.cos(x_phase)
    sine = jnp.sin(x_phase)
    return jnp.stack([jnp.stack([cosine, sine], axis=1), jnp.stack([-sine, cosine], axis=1)], axis=0)


def spectra_local(features):
    channels = features.shape[0]
    planes = features.shape[1]
    z_phase = phase_table(jnp.arange(Z, dtype=jnp.int32), jnp.arange(KZ, dtype=jnp.int32), Z)
    z_table = jnp.concatenate([jnp.cos(z_phase), -jnp.sin(z_phase)], axis=1).astype(jnp.bfloat16)
    flat = features.reshape(channels * planes * Y, Z)
    along_z = jnp.dot(flat, z_table, preferred_element_type=jnp.float32)
    stacked = along_z.reshape(channels, planes, Y, 2, KZ).transpose(3, 0, 1, 4, 2)
    y_phase = phase_table(jnp.arange(Y, dtype=jnp.int32), signed_modes(KY), Y)
    cosine = jnp.einsum('rcxky,yj->rcxjk', stacked, jnp.cos(y_phase), precision=lax.Precision.HIGHEST)
    sine = jnp.einsum('rcxky,yj->rcxjk', stacked, jnp.sin(y_phase), precision=lax.Precision.HIGHEST)
    real_part = cosine[0] + sine[1]
    imag_part = cosine[1] - sine[0]
    return jnp.stack([real_part, imag_part]).reshape(2, channels, planes, KY * KZ)


def along_first(partial_value, table):
    return jnp.einsum('rcxq,rxsk->qsck', partial_value, table, precision=lax.Precision.HIGHEST)


def contract(left, right):
    return jnp.einsum('im,iom->om', left, right, precision=lax.Precision.HIGHEST)


def mix_modes(spectrum, weights):
    real_part = contract(spectrum[0], weights[0]) - contract(spectrum[1], weights[1])
    imag_part = contract(spectrum[0], weights[1]) + contract(spectrum[1], weights[0])
    return jnp.stack([real_part, imag_part])


def back_first(blended, table):
    return jnp.einsum('rcqk,rxsk->scxq', blended, table, precision=lax.Precision.HIGHEST)


def finish_planes(spread, features, pointwise_weight, pointwise_bias):
    channels = features.shape[0]
    planes = features.shape[1]
    folded = spread.reshape(2, channels, planes, KY, KZ)
    y_phase = phase_table(jnp.arange(Y, dtype=jnp.int32), signed_modes(KY), Y)
    cosine = jnp.einsum('rcxjk,yj->rcxky', folded, jnp.cos(y_phase), precision=lax.Precision.HIGHEST)
    sine = jnp.einsum('rcxjk,yj->rcxky', folded, jnp.sin(y_phase), precision=lax.Precision.HIGHEST)
    halves = jnp.concatenate([cosine[0] - sine[1], sine[0] + cosine[1]], axis=2)
    z_phase = phase_table(jnp.arange(Z, dtype=jnp.int32), jnp.arange(KZ, dtype=jnp.int32), Z)
    factor = jnp.where(jnp.arange(KZ, dtype=jnp.int32) == 0, 1.0, 2.0).astype(jnp.float32) / (1.0 * X * Y * Z)
    z_table = jnp.concatenate([factor[:, None] * jnp.cos(z_phase).T, -factor[:, None] * jnp.sin(z_phase).T], axis=0)
    spectral = jnp.einsum('cxjy,jz->cxyz', halves, z_table, precision=lax.Precision.HIGHEST)
    linear = jnp.dot(pointwise_weight, features.reshape(channels, planes * Y * Z), preferred_element_type=jnp.float32).reshape(channels, planes, Y, Z)
    summed = spectral + linear + pointwise_bias[:, None, None, None]
    inner = 0.7978845608 * (summed + 0.044715 * summed * summed * summed)
    return (0.5 * summed * (1.0 + jnp.tanh(inner))).astype(jnp.bfloat16)


def reference(features, pointwise_weight, pointwise_bias, spectral_weight):
    indices = jnp.arange(X, dtype=jnp.int32)

    def forward_plane(plane_index):
        return spectra_local(lax.dynamic_slice_in_dim(features, plane_index, 1, 1))[:, :, 0, :]

    partial_value = jnp.moveaxis(lax.map(forward_plane, indices), 0, 2)
    spectrum = along_first(partial_value, forward_table(indices)).transpose(1, 2, 0, 3).reshape(2, C, KY * KZ * KX)
    blended = mix_modes(spectrum, spectral_weight).reshape(2, C, KY * KZ, KX)
    spread = back_first(blended, inverse_table(indices))

    def finish_plane(plane_index):
        return finish_planes(lax.dynamic_slice_in_dim(spread, plane_index, 1, 2), lax.dynamic_slice_in_dim(features, plane_index, 1, 1), pointwise_weight, pointwise_bias)[:, 0]

    return jnp.moveaxis(lax.map(finish_plane, indices), 0, 1)
```

```python
import functools
import math

import jax
import jax.numpy as jnp
import numpy as np
from jax import lax
from jax.experimental import pallas as pl
from jax.experimental.pallas import tpu as pltpu
from jax.sharding import PartitionSpec as P

KX = 32
KY = 32
KZ = 16
TWO_PI = 2.0 * math.pi
PACK = 8
F32 = jnp.float32
BF16 = jnp.bfloat16


def np_modes(number):
    ladder = np.arange(number)
    return np.where(ladder < number // 2, ladder, ladder - number)


def np_phase(positions, frequency, length):
    product = (positions[:, None] * frequency[None, :]) % length
    return product.astype(np.float64) * (TWO_PI / length)


def split_np(table):
    table = np.asarray(table, np.float32)
    high = table.astype(jnp.bfloat16)
    low = (table - high.astype(np.float32)).astype(jnp.bfloat16)
    return high, low


def split(value):
    high = value.astype(BF16)
    low = (value - high.astype(F32)).astype(BF16)
    return high, low


def dot(left, right):
    return jnp.dot(left, right, preferred_element_type=F32)


def lane_tiles(table):
    rows, lanes = table.shape
    pad = -lanes % 128
    table = np.pad(table, ((0, 0), (0, pad)))
    return np.ascontiguousarray(table.reshape(rows, -1, 128).transpose(1, 0, 2))


def wide(ref, rows=None):
    at = slice(None) if rows is None else rows
    return jnp.concatenate([ref[i, at, :] for i in range(ref.shape[0])], axis=1)


def tile_view(array):
    *lead, length_y, length_z = array.shape
    array = array.reshape(*lead, length_y // 8, 8, length_z // 128, 128)
    return jnp.swapaxes(array, -3, -2).reshape(*lead, length_y // 8, length_z // 16, 128)


def from_tile_view(array):
    *lead, blocks, rows, _ = array.shape
    array = array.reshape(*lead, blocks, rows // 8, 8, 128)
    return jnp.swapaxes(array, -3, -2).reshape(*lead, blocks * 8, rows * 16)


def rows_of(tiles):
    count, height, _ = tiles.shape
    tiles = tiles.astype(F32).reshape(count, height // 8, 8, 128)
    return jnp.concatenate([tiles[:, t].reshape(count * 8, 128) for t in range(height // 8)], axis=1)


def forward_tables(length_y, length_z):
    z_phase = np_phase(np.arange(length_z), np.arange(KZ), length_z)
    lanes = PACK * KZ
    z_tables = np.zeros((PACK, length_z, 2 * lanes), np.float32)
    for j in range(PACK):
        z_tables[j, :, j * KZ : (j + 1) * KZ] = np.cos(z_phase)
        z_tables[j, :, lanes + j * KZ : lanes + (j + 1) * KZ] = -np.sin(z_phase)
    y_phase = np_phase(np.arange(length_y), np_modes(KY), length_y).T
    high, low = split_np(np.concatenate([np.cos(y_phase), np.sin(y_phase)], axis=0))
    z_tables = z_tables.astype(jnp.bfloat16).astype(np.float32)
    return z_tables, lane_tiles(np.concatenate([high, low], axis=0))


def forward_body(rows, block_planes, feat_ref, z_ref, y_ref, out_ref):
    plane_at, group_at = pl.program_id(0), pl.program_id(1)
    groups = pl.num_programs(1)
    blocks, height = feat_ref.shape[2:4]
    length_y = blocks * 8
    lanes = PACK * KZ
    y_table = wide(y_ref)
    total = None
    for j in range(PACK):
        part = dot(rows_of(feat_ref[j].reshape(block_planes * blocks, height, 128)), z_ref[j])
        total = part if total is None else total + part
    for p in range(block_planes):
        high, low = split(total[p * length_y : (p + 1) * length_y])
        first = dot(y_table, high)
        both = first[: 2 * KY] + first[2 * KY :] + dot(y_table[: 2 * KY], low)
        cosine, sine = both[:KY], both[KY:]
        row = group_at * rows + (plane_at * block_planes + p) * 2
        out_ref[pl.ds(row, KY, stride=groups * rows), :] = cosine[:, :lanes] + sine[:, lanes:]
        out_ref[pl.ds(row + 1, KY, stride=groups * rows), :] = cosine[:, lanes:] - sine[:, :lanes]


def forward(features, block_planes):
    channels, planes, length_y, length_z = features.shape
    groups = channels // PACK
    rows = 2 * planes
    lanes = PACK * KZ
    z_tables, y_tables = forward_tables(length_y, length_z)
    tiles = tile_view(features)
    return pl.pallas_call(
        functools.partial(forward_body, rows, block_planes),
        out_shape=jax.ShapeDtypeStruct((KY * groups * rows, lanes), F32),
        grid=(planes // block_planes, groups),
        in_specs=[
            pl.BlockSpec((PACK, block_planes) + tiles.shape[2:], lambda p, g: (g, p, 0, 0, 0)),
            pl.BlockSpec(z_tables.shape, lambda p, g: (0, 0, 0)),
            pl.BlockSpec(y_tables.shape, lambda p, g: (0, 0, 0)),
        ],
        out_specs=pl.BlockSpec((KY * groups * rows, lanes), lambda p, g: (0, 0)),
        compiler_params=pltpu.CompilerParams(
            dimension_semantics=("arbitrary", "arbitrary"), vmem_limit_bytes=40 << 20
        ),
        name="forward_zy",
    )(tiles, jnp.asarray(z_tables), jnp.asarray(y_tables))


def middle_tables(length_x):
    phase = np_phase(np.arange(length_x), np_modes(KX), length_x)
    cosine, sine = np.cos(phase), np.sin(phase)
    ahead = np.zeros((2, KX, length_x, 2), np.float32)
    ahead[0, :, :, 0], ahead[0, :, :, 1] = cosine.T, sine.T
    ahead[1, :, :, 0], ahead[1, :, :, 1] = -sine.T, cosine.T
    high, low = split_np(ahead.reshape(2 * KX, 2 * length_x))
    back = np.zeros((length_x, 2, 2, KX), np.float32)
    back[:, 0, 0], back[:, 0, 1] = cosine, -sine
    back[:, 1, 0], back[:, 1, 1] = sine, cosine
    back_high, back_low = split_np(back.reshape(2 * length_x, 2 * KX))
    return (
        lane_tiles(np.concatenate([high, low], axis=0)),
        lane_tiles(np.concatenate([back_high, back_high, back_low], axis=1)),
    )


def regroup(pieces):
    count = len(pieces)
    width = pieces[0].shape[-1] // count
    group = lax.broadcasted_iota(jnp.int32, pieces[0].shape, 1) // width
    results = []
    for a in range(count):
        value = None
        for b in range(count):
            shift = ((b - a) * width) % (count * width)
            moved = pltpu.roll(pieces[b], shift, axis=1) if shift else pieces[b]
            value = moved if value is None else jnp.where(group == b, moved, value)
        results.append(value)
    return results


def middle_body(local, groups, in_ref, weight_ref, ahead_ref, back_ref, out_ref, turned, spec, mixed):
    devices, _, lanes = in_ref.shape
    rows = in_ref.shape[1] // (local * groups)
    channels = groups * PACK
    quarter = KZ // 4
    tables = wide(ahead_ref)
    back_table = wide(back_ref)[:, : 6 * KX]
    for g in range(groups):
        found = []
        for k in range(local):
            at = (k * groups + g) * rows
            high, low = split(in_ref[:, at : at + rows, :].reshape(devices * rows, lanes))
            first = dot(tables, high)
            found.append(first[: 2 * KX] + first[2 * KX :] + dot(tables[: 2 * KX], low))
        turned[...] = jnp.concatenate(found, axis=0).T
        for t in range(quarter):
            pieces = [turned[pl.ds(4 * t + j, PACK, stride=KZ), :] for j in range(4)]
            for a, value in enumerate(regroup(pieces)):
                k, r = a // 2, a % 2
                spec[r, g * PACK : (g + 1) * PACK, (k * quarter + t) * 128 : (k * quarter + t + 1) * 128] = value

    def mix(tile, carry):
        here = pl.ds(pl.multiple_of(tile * 128, 128), 128)
        real = imag = None
        for i in range(channels):
            s_real, s_imag = spec[0, i : i + 1, here], spec[1, i : i + 1, here]
            w_real, w_imag = weight_ref[0, i, :, here], weight_ref[1, i, :, here]
            add_real = s_real * w_real - s_imag * w_imag
            add_imag = s_real * w_imag + s_imag * w_real
            real = add_real if real is None else real + add_real
            imag = add_imag if imag is None else imag + add_imag
        mixed[0, :, here] = real
        mixed[1, :, here] = imag
        return carry

    lax.fori_loop(0, local * quarter, mix, 0)
    for g in range(groups):
        for t in range(quarter):
            pieces = [
                mixed[a % 2, g * PACK : (g + 1) * PACK, ((a // 2) * quarter + t) * 128 : ((a // 2) * quarter + t + 1) * 128]
                for a in range(4)
            ]
            for j, value in enumerate(regroup(pieces)):
                turned[pl.ds(4 * t + j, PACK, stride=KZ), :] = value
        modes = turned[...].T
        for k in range(local):
            high, low = split(modes[k * 2 * KX : (k + 1) * 2 * KX])
            spread = dot(back_table, jnp.concatenate([high, low, high], axis=0))
            at = (k * groups + g) * rows
            out_ref[:, at : at + rows, :] = spread.reshape(devices, rows, lanes)


def middle(gathered, spectral_weight, length_x, local, groups):
    channels = spectral_weight.shape[1]
    ahead, back = middle_tables(length_x)
    modes = spectral_weight.shape[3]
    whole = pl.BlockSpec(memory_space=pltpu.VMEM)
    return pl.pallas_call(
        functools.partial(middle_body, local, groups),
        out_shape=jax.ShapeDtypeStruct(gathered.shape, F32),
        in_specs=[whole] * 4,
        out_specs=whole,
        scratch_shapes=[
            pltpu.VMEM((PACK * KZ, local * 2 * KX), F32),
            pltpu.VMEM((2, channels, modes), F32),
            pltpu.VMEM((2, channels, modes), F32),
        ],
        compiler_params=pltpu.CompilerParams(vmem_limit_bytes=32 << 20),
        name="middle_x",
    )(gathered, spectral_weight, jnp.asarray(ahead), jnp.asarray(back))


def final_tables(length_x, length_y, length_z):
    y_phase = np_phase(np.arange(length_y), np_modes(KY), length_y)
    high, low = split_np(np.concatenate([np.cos(y_phase), np.sin(y_phase)], axis=1))
    y_table = np.concatenate([high, high, low], axis=1)
    z_phase = np_phase(np.arange(length_z), np.arange(KZ), length_z).T
    factor = np.where(np.arange(KZ) == 0, 1.0, 2.0)[:, None] * (0.5 / (1.0 * length_x * length_y * length_z))
    z_high, z_low = split_np(np.concatenate([factor * np.cos(z_phase), -factor * np.sin(z_phase)], axis=0))
    ones = np.zeros((2 * KZ, length_z), np.float32)
    ones[:3] = 1.0
    z_table = np.concatenate([z_high, z_high, z_low, ones.astype(jnp.bfloat16)], axis=0)
    lanes = PACK * KZ
    pick = np.zeros((2, lanes, 2, PACK, 4, 2, KZ), np.float32)
    kz = np.arange(KZ)
    for o in range(PACK):
        for copy in range(4):
            pick[0, o * KZ + kz, 0, o, copy, 0, kz] = 1.0
            pick[1, o * KZ + kz, 0, o, copy, 1, kz] = 1.0
            pick[1, o * KZ + kz, 1, o, copy, 0, kz] = -1.0
            pick[0, o * KZ + kz, 1, o, copy, 1, kz] = 1.0
    pick = pick.reshape(2 * lanes, 2 * PACK * lanes).astype(jnp.bfloat16)
    return lane_tiles(y_table), lane_tiles(z_table), lane_tiles(pick)


def final_body(rows, chunk, modes_ref, feat_ref, kron_ref, bias_ref, y_ref, z_ref, pick_ref, out_ref, picked, half):
    plane, part_at = pl.program_id(0), pl.program_id(1)
    channels = feat_ref.shape[0]
    groups = channels // PACK
    length_y = y_ref.shape[1]
    length_z = feat_ref.shape[3] * 16
    lanes = PACK * KZ

    @pl.when(part_at == 0)
    def prepare():
        stacked = []
        for g in range(groups):
            row = g * rows + plane * 2
            real = modes_ref[pl.ds(row, KY, stride=groups * rows), :]
            imag = modes_ref[pl.ds(row + 1, KY, stride=groups * rows), :]
            high, low = split(jnp.concatenate([real, imag], axis=1))
            stacked += [high, low]
        left = jnp.concatenate(stacked, axis=0)
        for at in range(0, 2 * PACK, 2):
            value = dot(left, jnp.concatenate([pick_ref[at], pick_ref[at + 1]], axis=1)).astype(BF16)
            picked[at] = value[:, :lanes]
            picked[at + 1] = value[:, lanes:]
        y_table = wide(y_ref)[:, : 6 * KY]
        lane = lax.broadcasted_iota(jnp.int32, (length_y // 8, 16, lanes), 2)
        for g in range(groups):
            high, low = 2 * g * KY, (2 * g + 1) * KY
            for pair in range(PACK // 2):
                parts = [
                    jnp.concatenate(
                        [picked[s * PACK + 2 * pair + i, h : h + KY, :] for h in (high, low, high) for s in range(2)],
                        axis=0,
                    )
                    for i in range(2)
                ]
                found = dot(y_table, jnp.concatenate(parts, axis=1))
                found = found.reshape(length_y // 8, 8, 2 * lanes)
                found = jnp.concatenate([found[:, :, :lanes], found[:, :, lanes:]], axis=1)
                top = found.astype(BF16)
                rest = (found - top.astype(F32)).astype(BF16)
                value = jnp.where(lane // (2 * KZ) == 1, rest, top)
                first = (g * PACK + 2 * pair) * 8
                value = jnp.where(lane < 6 * KZ, value, bias_ref[first : first + 16, :][None])
                half[:, first : first + 16, :] = value

    def block(b, carry):
        feats = rows_of(feat_ref[:, 0, b])
        h = dot(kron_ref[...], feats) + dot(half[part_at * (chunk // 8) + b], wide(z_ref))
        inner = h * (h * h * (8.0 * 0.7978845608 * 0.044715) + 2.0 * 0.7978845608)
        result = h * jnp.tanh(inner) + h
        result = result.reshape(channels, 8, length_z)
        parts = [result[:, :, t * 128 : (t + 1) * 128] for t in range(length_z // 128)]
        out_ref[:, 0, b] = jnp.concatenate(parts, axis=1).astype(BF16)
        return carry

    lax.fori_loop(0, chunk // 8, block, 0, unroll=8)


def final(spread, features, pointwise_weight, pointwise_bias, length_x, chunk):
    channels, planes, length_y, length_z = features.shape
    rows = 2 * planes
    groups = channels // PACK
    lanes = PACK * KZ
    y_table, z_table, pick = final_tables(length_x, length_y, length_z)
    kron = jnp.kron(0.5 * pointwise_weight.astype(F32), jnp.eye(8, dtype=F32))
    tiles = tile_view(features)
    bias = 0.5 * pointwise_bias
    b0 = lax.reduce_precision(bias, 8, 7)
    b1 = lax.reduce_precision(bias - b0, 8, 7)
    b2 = bias - b0 - b1
    pieces = jnp.stack([b0, b1, b2], axis=1)
    bias_rows = jnp.pad(pieces, ((0, 0), (6 * KZ, lanes - 6 * KZ - 3))).astype(BF16)
    bias_rows = jnp.repeat(bias_rows, 8, axis=0)

    def fixed(array):
        return pl.BlockSpec(array.shape, lambda p, q: (0,) * array.ndim)

    tables = [jnp.asarray(y_table), jnp.asarray(z_table), jnp.asarray(pick)]
    grid_block = pl.BlockSpec((channels, 1, chunk // 8, tiles.shape[3], 128), lambda p, q: (0, p, q, 0, 0))
    out = pl.pallas_call(
        functools.partial(final_body, rows, chunk),
        out_shape=jax.ShapeDtypeStruct(tiles.shape, BF16),
        grid=(planes, length_y // chunk),
        in_specs=[fixed(spread), grid_block, fixed(kron), fixed(bias_rows)] + [fixed(t) for t in tables],
        out_specs=grid_block,
        scratch_shapes=[
            pltpu.VMEM((2 * PACK, groups * 2 * KY, lanes), BF16),
            pltpu.VMEM((length_y // 8, channels * 8, lanes), BF16),
        ],
        compiler_params=pltpu.CompilerParams(
            dimension_semantics=("arbitrary", "arbitrary"), vmem_limit_bytes=48 << 20
        ),
        name="final_yz",
    )(spread, tiles, kron, bias_rows, *tables)
    return from_tile_view(out)


def fused(devices, features, pointwise_weight, pointwise_bias, spectral_weight):
    channels, planes = features.shape[:2]
    length_x = planes * devices
    local = KY // devices
    groups = channels // PACK
    rows = 2 * planes
    lanes = PACK * KZ
    shape = (devices, local * groups * rows, lanes)
    partial_value = forward(features, 4).reshape(shape)
    gathered = lax.all_to_all(partial_value, "px", split_axis=0, concat_axis=0)
    spread = middle(gathered, spectral_weight, length_x, local, groups)
    spread = lax.all_to_all(spread, "px", split_axis=0, concat_axis=0)
    spread = spread.reshape(KY * groups * rows, lanes)
    return final(spread, features, pointwise_weight, pointwise_bias, length_x, 128)


def signed_modes(number):
    ladder = jnp.arange(number, dtype=jnp.int32)
    return jnp.where(ladder < number // 2, ladder, ladder - number)


def phase_table(positions, frequency, length):
    product = positions[:, None] * frequency[None, :] % length
    return product.astype(jnp.float32) * (TWO_PI / length)


def forward_table(positions):
    x_phase = phase_table(positions, signed_modes(KX), positions.shape[0])
    cosine = jnp.cos(x_phase)
    sine = jnp.sin(x_phase)
    return jnp.stack(
        [jnp.stack([cosine, -sine], axis=1), jnp.stack([sine, cosine], axis=1)], axis=0
    )


def inverse_table(positions):
    x_phase = phase_table(positions, signed_modes(KX), positions.shape[0])
    cosine = jnp.cos(x_phase)
    sine = jnp.sin(x_phase)
    return jnp.stack(
        [jnp.stack([cosine, sine], axis=1), jnp.stack([-sine, cosine], axis=1)], axis=0
    )


def spectra_local(features):
    channels, planes, Y, Z = features.shape
    z_phase = phase_table(jnp.arange(Z, dtype=jnp.int32), jnp.arange(KZ, dtype=jnp.int32), Z)
    z_table = jnp.concatenate([jnp.cos(z_phase), -jnp.sin(z_phase)], axis=1).astype(jnp.bfloat16)
    flat = features.reshape(channels * planes * Y, Z)
    along_z = jnp.dot(flat, z_table, preferred_element_type=jnp.float32)
    stacked = along_z.reshape(channels, planes, Y, 2, KZ).transpose(3, 0, 1, 4, 2)
    y_phase = phase_table(jnp.arange(Y, dtype=jnp.int32), signed_modes(KY), Y)
    cosine = jnp.einsum(
        "rcxky,yj->rcxjk", stacked, jnp.cos(y_phase), precision=lax.Precision.HIGHEST
    )
    sine = jnp.einsum("rcxky,yj->rcxjk", stacked, jnp.sin(y_phase), precision=lax.Precision.HIGHEST)
    real_part = cosine[0] + sine[1]
    imag_part = cosine[1] - sine[0]
    return jnp.stack([real_part, imag_part]).reshape(2, channels, planes, KY * KZ)


def along_first(partial_value, table):
    return jnp.einsum("rcxq,rxsk->qsck", partial_value, table, precision=lax.Precision.HIGHEST)


def contract(left, right):
    return jnp.einsum("im,iom->om", left, right, precision=lax.Precision.HIGHEST)


def mix_modes(spectrum, weights):
    real_part = contract(spectrum[0], weights[0]) - contract(spectrum[1], weights[1])
    imag_part = contract(spectrum[0], weights[1]) + contract(spectrum[1], weights[0])
    return jnp.stack([real_part, imag_part])


def back_first(blended, table):
    return jnp.einsum("rcqk,rxsk->scxq", blended, table, precision=lax.Precision.HIGHEST)


def finish_planes(length_x, spread, features, pointwise_weight, pointwise_bias):
    channels, planes, Y, Z = features.shape
    X = length_x
    folded = spread.reshape(2, channels, planes, KY, KZ)
    y_phase = phase_table(jnp.arange(Y, dtype=jnp.int32), signed_modes(KY), Y)
    cosine = jnp.einsum(
        "rcxjk,yj->rcxky", folded, jnp.cos(y_phase), precision=lax.Precision.HIGHEST
    )
    sine = jnp.einsum("rcxjk,yj->rcxky", folded, jnp.sin(y_phase), precision=lax.Precision.HIGHEST)
    halves = jnp.concatenate([cosine[0] - sine[1], sine[0] + cosine[1]], axis=2)
    z_phase = phase_table(jnp.arange(Z, dtype=jnp.int32), jnp.arange(KZ, dtype=jnp.int32), Z)
    factor = jnp.where(jnp.arange(KZ, dtype=jnp.int32) == 0, 1.0, 2.0).astype(jnp.float32) / (
        1.0 * X * Y * Z
    )
    z_table = jnp.concatenate(
        [factor[:, None] * jnp.cos(z_phase).T, -factor[:, None] * jnp.sin(z_phase).T], axis=0
    )
    spectral = jnp.einsum("cxjy,jz->cxyz", halves, z_table, precision=lax.Precision.HIGHEST)
    linear = jnp.dot(
        pointwise_weight,
        features.reshape(channels, planes * Y * Z),
        preferred_element_type=jnp.float32,
    ).reshape(channels, planes, Y, Z)
    summed = spectral + linear + pointwise_bias[:, None, None, None]
    inner = 0.7978845608 * (summed + 0.044715 * summed * summed * summed)
    return (0.5 * summed * (1.0 + jnp.tanh(inner))).astype(jnp.bfloat16)


def plain(length_x, features, pointwise_weight, pointwise_bias, spectral_weight):
    every_plane = jnp.arange(length_x, dtype=jnp.int32)
    channels = features.shape[0]
    partial_value = spectra_local(features)
    gathered = lax.all_to_all(partial_value, "px", split_axis=3, concat_axis=2, tiled=True)
    spectrum = along_first(gathered, forward_table(every_plane)).transpose(1, 2, 0, 3)
    local_pairs = spectrum.shape[2]
    blended = mix_modes(
        spectrum.reshape(2, channels, local_pairs * KX), spectral_weight
    ).reshape(
        2, channels, local_pairs, KX
    )
    spread = lax.all_to_all(
        back_first(blended, inverse_table(every_plane)),
        "px",
        split_axis=2,
        concat_axis=3,
        tiled=True,
    )
    return finish_planes(length_x, spread, features, pointwise_weight, pointwise_bias)


def on_device(devices, features, pointwise_weight, pointwise_bias, spectral_weight):
    channels, planes, length_y, length_z = features.shape
    fits = (
        KY == 2 * devices
        and planes % 4 == 0
        and channels % PACK == 0
        and length_y % 128 == 0
        and length_z % 128 == 0
    )
    call = functools.partial(fused, devices) if fits else functools.partial(plain, planes * devices)
    return call(features, pointwise_weight, pointwise_bias, spectral_weight)


def solution(mesh):
    in_specs = (P(None, ("groups", "px"), None, None), P(), P(), P(None, None, None, "px"))
    out_specs = P(None, ("groups", "px"), None, None)
    return jax.shard_map(
        functools.partial(on_device, mesh.shape["px"]),
        mesh=mesh,
        in_specs=in_specs,
        out_specs=out_specs,
        check_vma=False,
    )
```

```python
import functools
import math

import jax
import jax.numpy as jnp
import numpy as np
from jax import lax
from jax.experimental import pallas as pl
from jax.experimental.pallas import tpu as pltpu
from jax.sharding import PartitionSpec as P

KX = 32
KY = 32
KZ = 16
TWO_PI = 2.0 * math.pi
UNROLL = 32
PACK = 8
F32 = jnp.float32
BF16 = jnp.bfloat16


def np_modes(number):
    ladder = np.arange(number)
    return np.where(ladder < number // 2, ladder, ladder - number)


def np_phase(positions, frequency, length):
    product = (positions[:, None] * frequency[None, :]) % length
    return product.astype(np.float64) * (TWO_PI / length)


def split_np(table):
    table = np.asarray(table, np.float32)
    high = table.astype(jnp.bfloat16)
    low = (table - high.astype(np.float32)).astype(jnp.bfloat16)
    return high, low


def split(value):
    high = value.astype(BF16)
    low = (value - high.astype(F32)).astype(BF16)
    return high, low


def dot(left, right):
    return jnp.dot(left, right, preferred_element_type=F32)


def lane_tiles(table):
    rows, lanes = table.shape
    pad = -lanes % 128
    table = np.pad(table, ((0, 0), (0, pad)))
    return np.ascontiguousarray(table.reshape(rows, -1, 128).transpose(1, 0, 2))


def wide(ref, rows=None):
    at = slice(None) if rows is None else rows
    return jnp.concatenate([ref[i, at, :] for i in range(ref.shape[0])], axis=1)


def tile_view(array):
    *lead, length_y, length_z = array.shape
    array = array.reshape(*lead, length_y // 8, 8, length_z // 128, 128)
    return jnp.swapaxes(array, -3, -2).reshape(*lead, length_y // 8, length_z // 16, 128)


def from_tile_view(array):
    *lead, blocks, rows, _ = array.shape
    array = array.reshape(*lead, blocks, rows // 8, 8, 128)
    return jnp.swapaxes(array, -3, -2).reshape(*lead, blocks * 8, rows * 16)


def rows_of(tiles):
    count, height, _ = tiles.shape
    tiles = tiles.astype(F32).reshape(count, height // 8, 8, 128)
    return jnp.concatenate([tiles[:, t].reshape(count * 8, 128) for t in range(height // 8)], axis=1)


def forward_tables(length_y, length_z):
    z_phase = np_phase(np.arange(length_z), np.arange(KZ), length_z)
    lanes = PACK * KZ
    z_tables = np.zeros((PACK, length_z, 2 * lanes), np.float32)
    for j in range(PACK):
        z_tables[j, :, j * KZ : (j + 1) * KZ] = np.cos(z_phase)
        z_tables[j, :, lanes + j * KZ : lanes + (j + 1) * KZ] = -np.sin(z_phase)
    y_phase = np_phase(np.arange(length_y), np_modes(KY), length_y).T
    high, low = split_np(np.concatenate([np.cos(y_phase), np.sin(y_phase)], axis=0))
    z_tables = np.stack([lane_tiles(table) for table in z_tables.astype(jnp.bfloat16)])
    return z_tables, lane_tiles(np.concatenate([high, low], axis=0))


def forward_body(rows, block_planes, feat_ref, z_ref, y_ref, out_ref):
    plane_at, group_at = pl.program_id(0), pl.program_id(1)
    groups = pl.num_programs(1)
    blocks, height = feat_ref.shape[2:4]
    length_y = blocks * 8
    lanes = PACK * KZ
    y_table = wide(y_ref)
    total = None
    for j in range(PACK):
        part = dot(rows_of(feat_ref[j].reshape(block_planes * blocks, height, 128)).astype(BF16), wide(z_ref.at[j]))
        total = part if total is None else total + part
    for p in range(block_planes):
        high, low = split(total[p * length_y : (p + 1) * length_y])
        first = dot(y_table, high)
        both = first[: 2 * KY] + first[2 * KY :] + dot(y_table[: 2 * KY], low)
        cosine, sine = both[:KY], both[KY:]
        row = group_at * rows + (plane_at * block_planes + p) * 2
        out_ref[pl.ds(row, KY, stride=groups * rows), :] = cosine[:, :lanes] + sine[:, lanes:]
        out_ref[pl.ds(row + 1, KY, stride=groups * rows), :] = cosine[:, lanes:] - sine[:, :lanes]


def forward(features, block_planes):
    channels, planes, length_y, length_z = features.shape
    groups = channels // PACK
    rows = 2 * planes
    lanes = PACK * KZ
    z_tables, y_tables = forward_tables(length_y, length_z)
    tiles = tile_view(features)
    return pl.pallas_call(
        functools.partial(forward_body, rows, block_planes),
        out_shape=jax.ShapeDtypeStruct((KY * groups * rows, lanes), F32),
        grid=(planes // block_planes, groups),
        in_specs=[
            pl.BlockSpec((PACK, block_planes) + tiles.shape[2:], lambda p, g: (g, p, 0, 0, 0)),
            pl.BlockSpec(z_tables.shape, lambda p, g: (0, 0, 0, 0)),
            pl.BlockSpec(y_tables.shape, lambda p, g: (0, 0, 0)),
        ],
        out_specs=pl.BlockSpec((KY * groups * rows, lanes), lambda p, g: (0, 0)),
        compiler_params=pltpu.CompilerParams(
            dimension_semantics=("arbitrary", "arbitrary"), vmem_limit_bytes=40 << 20
        ),
        name="forward_zy",
    )(
        tiles,
        pltpu.with_memory_space_constraint(jnp.asarray(z_tables), pltpu.HBM),
        pltpu.with_memory_space_constraint(jnp.asarray(y_tables), pltpu.HBM),
    )


def middle_tables(length_x):
    phase = np_phase(np.arange(length_x), np_modes(KX), length_x)
    cosine, sine = np.cos(phase), np.sin(phase)
    ahead = np.zeros((2, KX, length_x, 2), np.float32)
    ahead[0, :, :, 0], ahead[0, :, :, 1] = cosine.T, sine.T
    ahead[1, :, :, 0], ahead[1, :, :, 1] = -sine.T, cosine.T
    high, low = split_np(ahead.reshape(2 * KX, 2 * length_x))
    back = np.zeros((length_x, 2, 2, KX), np.float32)
    back[:, 0, 0], back[:, 0, 1] = cosine, -sine
    back[:, 1, 0], back[:, 1, 1] = sine, cosine
    back_high, back_low = split_np(back.reshape(2 * length_x, 2 * KX))
    return (
        lane_tiles(np.concatenate([high, low], axis=0)),
        lane_tiles(np.concatenate([back_high, back_high, back_low], axis=1)),
    )


def regroup(pieces):
    count = len(pieces)
    width = pieces[0].shape[-1] // count
    group = lax.broadcasted_iota(jnp.int32, pieces[0].shape, 1) // width
    results = []
    for a in range(count):
        value = None
        for b in range(count):
            shift = ((b - a) * width) % (count * width)
            moved = pltpu.roll(pieces[b], shift, axis=1) if shift else pieces[b]
            value = moved if value is None else jnp.where(group == b, moved, value)
        results.append(value)
    return results


def middle_body(local, groups, parts, in_ref, weight_ref, ahead_ref, back_ref, *rest):
    out_refs, (turned, spec, mixed) = rest[:parts], rest[parts:]
    devices, _, lanes = in_ref.shape
    rows = in_ref.shape[1] // (local * groups)
    channels = groups * PACK
    quarter = KZ // 4
    tables = wide(ahead_ref)
    back_table = wide(back_ref)[:, : 6 * KX]
    for g in range(groups):
        found = []
        for k in range(local):
            at = (k * groups + g) * rows
            high, low = split(in_ref[:, at : at + rows, :].reshape(devices * rows, lanes))
            first = dot(tables, high)
            found.append(first[: 2 * KX] + first[2 * KX :] + dot(tables[: 2 * KX], low))
        turned[...] = jnp.concatenate(found, axis=0).T
        for t in range(quarter):
            pieces = [turned[pl.ds(4 * t + j, PACK, stride=KZ), :] for j in range(4)]
            for a, value in enumerate(regroup(pieces)):
                k, r = a // 2, a % 2
                spec[r, g * PACK : (g + 1) * PACK, (k * quarter + t) * 128 : (k * quarter + t + 1) * 128] = value

    def mix(tile, carry):
        here = pl.ds(pl.multiple_of(tile * 128, 128), 128)
        real = imag = None
        for i in range(channels):
            s_real, s_imag = spec[0, i : i + 1, here], spec[1, i : i + 1, here]
            w_real, w_imag = weight_ref[0, i, :, here], weight_ref[1, i, :, here]
            add_real = s_real * w_real - s_imag * w_imag
            add_imag = s_real * w_imag + s_imag * w_real
            real = add_real if real is None else real + add_real
            imag = add_imag if imag is None else imag + add_imag
        mixed[0, :, here] = real
        mixed[1, :, here] = imag
        return carry

    lax.fori_loop(0, local * quarter, mix, 0)
    for g in range(groups):
        for t in range(quarter):
            pieces = [
                mixed[a % 2, g * PACK : (g + 1) * PACK, ((a // 2) * quarter + t) * 128 : ((a // 2) * quarter + t + 1) * 128]
                for a in range(4)
            ]
            for j, value in enumerate(regroup(pieces)):
                turned[pl.ds(4 * t + j, PACK, stride=KZ), :] = value
        modes = turned[...].T
        for k in range(local):
            high, low = split(modes[k * 2 * KX : (k + 1) * 2 * KX])
            spread = dot(back_table, jnp.concatenate([high, low, high], axis=0))
            spread = spread.reshape(devices, rows, lanes)
            size = rows // parts
            at = (k * groups + g) * size
            for part, out_ref in enumerate(out_refs):
                out_ref[:, at : at + size, :] = spread[:, part * size : (part + 1) * size]


def middle(gathered, spectral_weight, length_x, local, groups, parts):
    channels = spectral_weight.shape[1]
    ahead, back = middle_tables(length_x)
    modes = spectral_weight.shape[3]
    whole = pl.BlockSpec(memory_space=pltpu.VMEM)
    return pl.pallas_call(
        functools.partial(middle_body, local, groups, parts),
        out_shape=[jax.ShapeDtypeStruct((gathered.shape[0], gathered.shape[1] // parts, gathered.shape[2]), F32)] * parts,
        in_specs=[whole] * 4,
        out_specs=[whole] * parts,
        scratch_shapes=[
            pltpu.VMEM((PACK * KZ, local * 2 * KX), F32),
            pltpu.VMEM((2, channels, modes), F32),
            pltpu.VMEM((2, channels, modes), F32),
        ],
        compiler_params=pltpu.CompilerParams(vmem_limit_bytes=32 << 20),
        name="middle_x",
    )(gathered, spectral_weight, jnp.asarray(ahead), jnp.asarray(back))


def final_tables(length_x, length_y, length_z):
    y_phase = np_phase(np.arange(length_y), np_modes(KY), length_y)
    high, low = split_np(np.concatenate([np.cos(y_phase), np.sin(y_phase)], axis=1))
    ones = np.zeros((length_y, 16), np.float32)
    ones[:, :3] = 1.0
    y_table = np.concatenate([high, high, low, ones.astype(jnp.bfloat16)], axis=1)
    z_phase = np_phase(np.arange(length_z), np.arange(KZ), length_z).T
    factor = np.where(np.arange(KZ) == 0, 1.0, 2.0)[:, None] * (0.5 / (1.0 * length_x * length_y * length_z))
    z_high, z_low = split_np(np.concatenate([factor * np.cos(z_phase), -factor * np.sin(z_phase)], axis=0))
    z_table = np.zeros((2, 256, length_z), jnp.bfloat16)
    for slot in range(2):
        at = slot * 64
        z_table[slot, at : at + 32] = z_high
        z_table[slot, at + 32 : at + 64] = z_low
        z_table[slot, 128 + at : 128 + at + 32] = z_high
    lanes = PACK * KZ
    pick = np.zeros((2, lanes, 2, PACK, 2, 2, KZ), np.float32)
    kz = np.arange(KZ)
    for o in range(PACK):
        for copy in range(2):
            pick[0, o * KZ + kz, 0, o, copy, 0, kz] = 1.0
            pick[1, o * KZ + kz, 0, o, copy, 1, kz] = 1.0
            pick[1, o * KZ + kz, 1, o, copy, 0, kz] = -1.0
            pick[0, o * KZ + kz, 1, o, copy, 1, kz] = 1.0
    pick = pick.reshape(2 * lanes, PACK * lanes).astype(jnp.bfloat16)
    return lane_tiles(y_table), np.stack([lane_tiles(table) for table in z_table]), lane_tiles(pick)


def final_body(rows, chunk, modes_ref, feat_ref, kron_ref, bias_ref, y_ref, z_ref, pick_ref, *rest):
    out_ref, picked, half = rest[-3:]
    plane, part_at = pl.program_id(0), pl.program_id(1)
    channels = feat_ref.shape[0]
    groups = channels // PACK
    length_y = y_ref.shape[1]
    length_z = feat_ref.shape[3] * 16
    lanes = PACK * KZ
    pairs = PACK // 2

    @pl.when(part_at == 0)
    def prepare():
        stacked = []
        for g in range(groups):
            row = g * rows + plane * 2
            real = modes_ref[pl.ds(row, KY, stride=groups * rows), :]
            imag = modes_ref[pl.ds(row + 1, KY, stride=groups * rows), :]
            high, low = split(jnp.concatenate([real, imag], axis=1))
            stacked += [high, low]
        left = jnp.concatenate(stacked, axis=0)
        for at in range(0, 2 * pairs, 2):
            value = dot(left, jnp.concatenate([pick_ref[at], pick_ref[at + 1]], axis=1)).astype(BF16)
            picked[at] = value[:, :lanes]
            picked[at + 1] = value[:, lanes:]
        y_table = wide(y_ref)[:, : 6 * KY + 16]
        for g in range(groups):
            high, low = 2 * g * KY, (2 * g + 1) * KY
            for f in range(pairs // 2):
                parts = [
                    jnp.concatenate(
                        [picked[s * pairs + 2 * f + t, h : h + KY, :] for h in (high, low, high) for s in range(2)]
                        + [bias_ref[g * pairs + 2 * f + t]],
                        axis=0,
                    )
                    for t in range(2)
                ]
                found = dot(y_table, jnp.concatenate(parts, axis=1))
                found = found.reshape(length_y // 8, 8, 2 * lanes)
                found = jnp.concatenate([found[:, :, :lanes], found[:, :, lanes:]], axis=1)
                top = found.astype(BF16)
                first = (g * pairs + 2 * f) * 8
                half[0, :, first : first + 16, :] = top
                half[1, :, first : first + 16, :] = (found - top.astype(F32)).astype(BF16)

    kron = wide(kron_ref)
    z_tables = [wide(z_ref.at[slot]) for slot in range(2)]
    size = channels * 4

    def block(b, carry):
        feats = rows_of(feat_ref[:, 0, b]).astype(BF16)
        at = part_at * (chunk // 8) + b
        left = jnp.concatenate([half[0, at], half[1, at]], axis=1)
        for slot in range(2):
            h = dot(kron[slot * size : (slot + 1) * size], feats) + dot(left, z_tables[slot])
            inner = h * (h * h * (8.0 * 0.7978845608 * 0.044715) + 2.0 * 0.7978845608)
            result = (h * jnp.tanh(inner) + h).reshape(channels // 2, 8, length_z)
            parts = [result[:, :, t * 128 : (t + 1) * 128] for t in range(length_z // 128)]
            result = jnp.concatenate(parts, axis=1).astype(BF16)
            for i in range(channels // 2):
                out_ref[2 * i + slot, 0, b] = result[i]
        return carry

    lax.fori_loop(0, chunk // 8, block, 0, unroll=UNROLL)


def final_operands(features, pointwise_weight, pointwise_bias, length_x):
    length_y, length_z = features.shape[2:]
    lanes = PACK * KZ
    tables = [jnp.asarray(table) for table in final_tables(length_x, length_y, length_z)]
    channels = features.shape[0]
    weight = 0.5 * pointwise_weight.astype(F32)
    weight = weight.reshape(channels // 2, 2, channels).swapaxes(0, 1).reshape(channels, channels)
    kron = jnp.kron(weight, jnp.eye(8, dtype=F32)).astype(BF16)
    kron = kron.reshape(channels * 8, channels // 16, 128).swapaxes(0, 1)
    bias = pointwise_bias * (1.0 * length_x * length_y * length_z)
    b0 = lax.reduce_precision(bias, 8, 7)
    b1 = lax.reduce_precision(bias - b0, 8, 7)
    b2 = bias - b0 - b1
    pieces = jnp.stack([b0, b1, b2], axis=0).reshape(3, channels // 2, 2).swapaxes(0, 1).astype(BF16)
    pieces = jnp.pad(pieces[:, :, :, None, None], ((0, 0), (0, 13), (0, 0), (0, 0), (0, 31)))
    pieces = jnp.broadcast_to(pieces, (channels // 2, 16, 2, 2, 32)).reshape(channels // 2, 16, lanes)
    return [kron, pieces] + tables


def final(spread, tiles, operands, first_plane, count, chunk, before):
    channels, planes, blocks = tiles.shape[:3]
    rows = 2 * count
    groups = channels // PACK
    lanes = PACK * KZ

    def fixed(array):
        return pl.BlockSpec(array.shape, lambda p, q: (0,) * array.ndim)

    grid_block = pl.BlockSpec(
        (channels, 1, chunk // 8, tiles.shape[3], 128), lambda p, q: (0, p + first_plane, q, 0, 0)
    )
    in_specs = [fixed(spread), grid_block] + [fixed(operand) for operand in operands]
    arguments = [spread, tiles] + operands
    aliases = {}
    if before is not None:
        aliases = {len(arguments): 0}
        in_specs.append(pl.BlockSpec(memory_space=pl.ANY))
        arguments.append(before)
    points = channels * count * blocks * 8 * tiles.shape[3] * 16
    return pl.pallas_call(
        functools.partial(final_body, rows, chunk),
        out_shape=jax.ShapeDtypeStruct(tiles.shape, BF16),
        grid=(count, blocks * 8 // chunk),
        in_specs=in_specs,
        out_specs=grid_block,
        scratch_shapes=[
            pltpu.VMEM((PACK, groups * 2 * KY, lanes), BF16),
            pltpu.VMEM((2, blocks, channels * 4, lanes), BF16),
        ],
        input_output_aliases=aliases,
        cost_estimate=pl.CostEstimate(flops=points * 2000, bytes_accessed=4 * points, transcendentals=points),
        compiler_params=pltpu.CompilerParams(
            dimension_semantics=("arbitrary", "arbitrary"), vmem_limit_bytes=48 << 20
        ),
        name="final_yz",
    )(*arguments)


def fused(devices, features, pointwise_weight, pointwise_bias, spectral_weight):
    channels, planes = features.shape[:2]
    length_x = planes * devices
    local = KY // devices
    groups = channels // PACK
    rows = 2 * planes
    lanes = PACK * KZ
    shape = (devices, local * groups * rows, lanes)
    partial_value = forward(features, 4).reshape(shape)
    gathered = lax.all_to_all(partial_value, "px", split_axis=0, concat_axis=0)
    parts = 2
    count = planes // parts
    spreads = middle(gathered, spectral_weight, length_x, local, groups, parts)
    tiles = tile_view(features)
    operands = final_operands(features, pointwise_weight, pointwise_bias, length_x)
    arrived, out = None, None
    ready = []
    for spread in spreads:
        if arrived is not None:
            spread, arrived = lax.optimization_barrier((spread, arrived))
            ready[-1] = arrived
        arrived = lax.all_to_all(spread, "px", split_axis=0, concat_axis=0)
        ready.append(arrived)
    for part, spread in enumerate(ready):
        spread = spread.reshape(KY * groups * 2 * count, lanes)
        out = final(spread, tiles, operands, part * count, count, 256, out)
    return from_tile_view(out)


def signed_modes(number):
    ladder = jnp.arange(number, dtype=jnp.int32)
    return jnp.where(ladder < number // 2, ladder, ladder - number)


def phase_table(positions, frequency, length):
    product = positions[:, None] * frequency[None, :] % length
    return product.astype(jnp.float32) * (TWO_PI / length)


def forward_table(positions):
    x_phase = phase_table(positions, signed_modes(KX), positions.shape[0])
    cosine = jnp.cos(x_phase)
    sine = jnp.sin(x_phase)
    return jnp.stack(
        [jnp.stack([cosine, -sine], axis=1), jnp.stack([sine, cosine], axis=1)], axis=0
    )


def inverse_table(positions):
    x_phase = phase_table(positions, signed_modes(KX), positions.shape[0])
    cosine = jnp.cos(x_phase)
    sine = jnp.sin(x_phase)
    return jnp.stack(
        [jnp.stack([cosine, sine], axis=1), jnp.stack([-sine, cosine], axis=1)], axis=0
    )


def spectra_local(features):
    channels, planes, Y, Z = features.shape
    z_phase = phase_table(jnp.arange(Z, dtype=jnp.int32), jnp.arange(KZ, dtype=jnp.int32), Z)
    z_table = jnp.concatenate([jnp.cos(z_phase), -jnp.sin(z_phase)], axis=1).astype(jnp.bfloat16)
    flat = features.reshape(channels * planes * Y, Z)
    along_z = jnp.dot(flat, z_table, preferred_element_type=jnp.float32)
    stacked = along_z.reshape(channels, planes, Y, 2, KZ).transpose(3, 0, 1, 4, 2)
    y_phase = phase_table(jnp.arange(Y, dtype=jnp.int32), signed_modes(KY), Y)
    cosine = jnp.einsum(
        "rcxky,yj->rcxjk", stacked, jnp.cos(y_phase), precision=lax.Precision.HIGHEST
    )
    sine = jnp.einsum("rcxky,yj->rcxjk", stacked, jnp.sin(y_phase), precision=lax.Precision.HIGHEST)
    real_part = cosine[0] + sine[1]
    imag_part = cosine[1] - sine[0]
    return jnp.stack([real_part, imag_part]).reshape(2, channels, planes, KY * KZ)


def along_first(partial_value, table):
    return jnp.einsum("rcxq,rxsk->qsck", partial_value, table, precision=lax.Precision.HIGHEST)


def contract(left, right):
    return jnp.einsum("im,iom->om", left, right, precision=lax.Precision.HIGHEST)


def mix_modes(spectrum, weights):
    real_part = contract(spectrum[0], weights[0]) - contract(spectrum[1], weights[1])
    imag_part = contract(spectrum[0], weights[1]) + contract(spectrum[1], weights[0])
    return jnp.stack([real_part, imag_part])


def back_first(blended, table):
    return jnp.einsum("rcqk,rxsk->scxq", blended, table, precision=lax.Precision.HIGHEST)


def finish_planes(length_x, spread, features, pointwise_weight, pointwise_bias):
    channels, planes, Y, Z = features.shape
    X = length_x
    folded = spread.reshape(2, channels, planes, KY, KZ)
    y_phase = phase_table(jnp.arange(Y, dtype=jnp.int32), signed_modes(KY), Y)
    cosine = jnp.einsum(
        "rcxjk,yj->rcxky", folded, jnp.cos(y_phase), precision=lax.Precision.HIGHEST
    )
    sine = jnp.einsum("rcxjk,yj->rcxky", folded, jnp.sin(y_phase), precision=lax.Precision.HIGHEST)
    halves = jnp.concatenate([cosine[0] - sine[1], sine[0] + cosine[1]], axis=2)
    z_phase = phase_table(jnp.arange(Z, dtype=jnp.int32), jnp.arange(KZ, dtype=jnp.int32), Z)
    factor = jnp.where(jnp.arange(KZ, dtype=jnp.int32) == 0, 1.0, 2.0).astype(jnp.float32) / (
        1.0 * X * Y * Z
    )
    z_table = jnp.concatenate(
        [factor[:, None] * jnp.cos(z_phase).T, -factor[:, None] * jnp.sin(z_phase).T], axis=0
    )
    spectral = jnp.einsum("cxjy,jz->cxyz", halves, z_table, precision=lax.Precision.HIGHEST)
    linear = jnp.dot(
        pointwise_weight,
        features.reshape(channels, planes * Y * Z),
        preferred_element_type=jnp.float32,
    ).reshape(channels, planes, Y, Z)
    summed = spectral + linear + pointwise_bias[:, None, None, None]
    inner = 0.7978845608 * (summed + 0.044715 * summed * summed * summed)
    return (0.5 * summed * (1.0 + jnp.tanh(inner))).astype(jnp.bfloat16)


def plain(length_x, features, pointwise_weight, pointwise_bias, spectral_weight):
    every_plane = jnp.arange(length_x, dtype=jnp.int32)
    channels = features.shape[0]
    partial_value = spectra_local(features)
    gathered = lax.all_to_all(partial_value, "px", split_axis=3, concat_axis=2, tiled=True)
    spectrum = along_first(gathered, forward_table(every_plane)).transpose(1, 2, 0, 3)
    local_pairs = spectrum.shape[2]
    blended = mix_modes(
        spectrum.reshape(2, channels, local_pairs * KX), spectral_weight
    ).reshape(
        2, channels, local_pairs, KX
    )
    spread = lax.all_to_all(
        back_first(blended, inverse_table(every_plane)),
        "px",
        split_axis=2,
        concat_axis=3,
        tiled=True,
    )
    return finish_planes(length_x, spread, features, pointwise_weight, pointwise_bias)


def on_device(devices, features, pointwise_weight, pointwise_bias, spectral_weight):
    channels, planes, length_y, length_z = features.shape
    fits = (
        KY == 2 * devices
        and planes % 8 == 0
        and channels == 32
        and length_y % 128 == 0
        and length_z == 256
    )
    call = functools.partial(fused, devices) if fits else functools.partial(plain, planes * devices)
    return call(features, pointwise_weight, pointwise_bias, spectral_weight)


def solution(mesh):
    in_specs = (P(None, ("groups", "px"), None, None), P(), P(), P(None, None, None, "px"))
    out_specs = P(None, ("groups", "px"), None, None)
    return jax.shard_map(
        functools.partial(on_device, mesh.shape["px"]),
        mesh=mesh,
        in_specs=in_specs,
        out_specs=out_specs,
        check_vma=False,
    )
```

```python
import functools
import math

import jax
import jax.numpy as jnp
import numpy as np
from jax import lax
from jax.experimental import pallas as pl
from jax.experimental.pallas import tpu as pltpu
from jax.sharding import PartitionSpec as P

KX = 32
KY = 32
KZ = 16
TWO_PI = 2.0 * math.pi
PARTS = 2
PIECES = 4
PACK = 8
F32 = jnp.float32
BF16 = jnp.bfloat16


def np_modes(number):
    ladder = np.arange(number)
    return np.where(ladder < number // 2, ladder, ladder - number)


def np_phase(positions, frequency, length):
    product = (positions[:, None] * frequency[None, :]) % length
    return product.astype(np.float64) * (TWO_PI / length)


def split_np(table):
    table = np.asarray(table, np.float32)
    high = table.astype(jnp.bfloat16)
    low = (table - high.astype(np.float32)).astype(jnp.bfloat16)
    return high, low


def split(value):
    high = value.astype(BF16)
    low = (value - high.astype(F32)).astype(BF16)
    return high, low


def dot(left, right):
    return jnp.dot(left, right, preferred_element_type=F32)


def lane_tiles(table):
    rows, lanes = table.shape
    pad = -lanes % 128
    table = np.pad(table, ((0, 0), (0, pad)))
    return np.ascontiguousarray(table.reshape(rows, -1, 128).transpose(1, 0, 2))


def wide(ref, rows=None):
    at = slice(None) if rows is None else rows
    return jnp.concatenate([ref[i, at, :] for i in range(ref.shape[0])], axis=1)


def tile_view(array):
    *lead, length_y, length_z = array.shape
    array = array.reshape(*lead, length_y // 8, 8, length_z // 128, 128)
    return jnp.swapaxes(array, -3, -2).reshape(*lead, length_y // 8, length_z // 16, 128)


def from_tile_view(array):
    *lead, blocks, rows, _ = array.shape
    array = array.reshape(*lead, blocks, rows // 8, 8, 128)
    return jnp.swapaxes(array, -3, -2).reshape(*lead, blocks * 8, rows * 16)


def rows_of(tiles):
    count, height, _ = tiles.shape
    tiles = tiles.astype(F32).reshape(count, height // 8, 8, 128)
    return jnp.concatenate([tiles[:, t].reshape(count * 8, 128) for t in range(height // 8)], axis=1)


def forward_tables(length_y, length_z):
    z_phase = np_phase(np.arange(length_z), np.arange(KZ), length_z)
    lanes = PACK * KZ
    z_tables = np.zeros((PACK, length_z, 2 * lanes), np.float32)
    for j in range(PACK):
        z_tables[j, :, j * KZ : (j + 1) * KZ] = np.cos(z_phase)
        z_tables[j, :, lanes + j * KZ : lanes + (j + 1) * KZ] = -np.sin(z_phase)
    y_phase = np_phase(np.arange(length_y), np_modes(KY), length_y).T
    high, low = split_np(np.concatenate([np.cos(y_phase), np.sin(y_phase)], axis=0))
    z_tables = np.stack([lane_tiles(table) for table in z_tables.astype(jnp.bfloat16)])
    return z_tables, lane_tiles(np.concatenate([high, low], axis=0))


def forward_body(first_plane, block_planes, feat_ref, z_from, y_from, out_ref, held, arrivals, z_ref, y_ref, tables):
    channels, planes, blocks, height = held.shape[:4]
    length_y = blocks * 8
    lanes = PACK * KZ
    groups = channels // PACK
    rows = 2 * planes
    copies = [
        pltpu.make_async_copy(z_from, z_ref, tables.at[0]),
        pltpu.make_async_copy(y_from, y_ref, tables.at[1]),
    ]

    def load(step):
        across, along = pl.ds((step % groups) * PACK, PACK), (step // groups) * block_planes
        return pltpu.make_async_copy(
            feat_ref.at[across, pl.ds(first_plane + along, block_planes)],
            held.at[across, pl.ds(along, block_planes)],
            arrivals.at[step],
        )

    steps = groups * (planes // block_planes)
    for copy in copies:
        copy.start()
    load(0).start()
    for copy in copies:
        copy.wait()
    y_table = wide(y_ref)

    def one(step, carry):
        group_at, plane_at = step % groups, step // groups
        load(step).wait()

        @pl.when(step == 0)
        def second():
            load(1).start()

        @pl.when(step + 2 < steps)
        def ahead():
            load(step + 2).start()

        total = None
        for j in range(PACK):
            tiles = held[group_at * PACK + j, pl.ds(plane_at * block_planes, block_planes)]
            left = rows_of(tiles.reshape(block_planes * blocks, height, 128)).astype(BF16)
            part = dot(left, wide(z_ref.at[j]))
            total = part if total is None else total + part
        for p in range(block_planes):
            high, low = split(total[p * length_y : (p + 1) * length_y])
            first = dot(y_table, high)
            both = first[: 2 * KY] + first[2 * KY :] + dot(y_table[: 2 * KY], low)
            cosine, sine = both[:KY], both[KY:]
            row = group_at * rows + (plane_at * block_planes + p) * 2
            out_ref[pl.ds(row, KY, stride=groups * rows), :] = cosine[:, :lanes] + sine[:, lanes:]
            out_ref[pl.ds(row + 1, KY, stride=groups * rows), :] = cosine[:, lanes:] - sine[:, :lanes]
        return carry

    lax.fori_loop(0, steps, one, 0)


def forward(tiles, first_plane, planes, block_planes):
    channels, _, blocks, height = tiles.shape[:4]
    groups = channels // PACK
    lanes = PACK * KZ
    z_tables, y_tables = forward_tables(blocks * 8, height * 16)
    steps = groups * (planes // block_planes)
    whole = pl.BlockSpec(memory_space=pltpu.VMEM)
    points = channels * planes * blocks * 8 * height * 16
    return pl.pallas_call(
        functools.partial(forward_body, first_plane, block_planes),
        out_shape=jax.ShapeDtypeStruct((KY * groups * 2 * planes, lanes), F32),
        in_specs=[pl.BlockSpec(memory_space=pltpu.HBM)] * 3,
        out_specs=whole,
        scratch_shapes=[
            pltpu.VMEM((channels, planes) + tiles.shape[2:], BF16),
            pltpu.SemaphoreType.DMA((steps,)),
            pltpu.VMEM(z_tables.shape, BF16),
            pltpu.VMEM(y_tables.shape, BF16),
            pltpu.SemaphoreType.DMA((2,)),
        ],
        cost_estimate=pl.CostEstimate(flops=points * 1000, bytes_accessed=2 * points, transcendentals=0),
        compiler_params=pltpu.CompilerParams(vmem_limit_bytes=44 << 20),
        name="forward_zy",
    )(
        pltpu.with_memory_space_constraint(tiles, pltpu.HBM),
        pltpu.with_memory_space_constraint(jnp.asarray(z_tables), pltpu.HBM),
        pltpu.with_memory_space_constraint(jnp.asarray(y_tables), pltpu.HBM),
    )


def middle_tables(length_x):
    phase = np_phase(np.arange(length_x), np_modes(KX), length_x)
    cosine, sine = np.cos(phase), np.sin(phase)
    ahead = np.zeros((2, KX, length_x, 2), np.float32)
    ahead[0, :, :, 0], ahead[0, :, :, 1] = cosine.T, sine.T
    ahead[1, :, :, 0], ahead[1, :, :, 1] = -sine.T, cosine.T
    high, low = split_np(ahead.reshape(2 * KX, 2 * length_x))
    back = np.zeros((length_x, 2, 2, KX), np.float32)
    back[:, 0, 0], back[:, 0, 1] = cosine, -sine
    back[:, 1, 0], back[:, 1, 1] = sine, cosine
    back_high, back_low = split_np(back.reshape(2 * length_x, 2 * KX))
    return (
        lane_tiles(np.concatenate([high, low], axis=0)),
        lane_tiles(np.concatenate([back_high, back_high, back_low], axis=1)),
    )


def regroup(pieces):
    count = len(pieces)
    width = pieces[0].shape[-1] // count
    group = lax.broadcasted_iota(jnp.int32, pieces[0].shape, 1) // width
    results = []
    for a in range(count):
        value = None
        for b in range(count):
            shift = ((b - a) * width) % (count * width)
            moved = pltpu.roll(pieces[b], shift, axis=1) if shift else pieces[b]
            value = moved if value is None else jnp.where(group == b, moved, value)
        results.append(value)
    return results


def middle_body(local, groups, parts, in_ref, weight_ref, ahead_ref, back_ref, *refs):
    out_refs, (turned, spec, mixed, weights, arrivals) = refs[:parts], refs[parts:]
    weight_tiles = weights.shape[0]

    def load(tile):
        here = pl.ds(pl.multiple_of(tile * 128, 128), 128)
        return pltpu.make_async_copy(weight_ref.at[:, :, :, here], weights.at[tile], arrivals.at[tile])

    for tile in range(weight_tiles):
        load(tile).start()
    devices, _, lanes = in_ref.shape
    rows = in_ref.shape[1] // (local * groups)
    size = rows // parts
    channels = groups * PACK
    quarter = KZ // 4
    tables = wide(ahead_ref)
    back_table = wide(back_ref)[:, : 6 * KX]
    for g in range(groups):
        found = []
        for k in range(local):
            at = (k * groups + g) * rows
            high, low = split(in_ref[:, at : at + rows, :].reshape(devices * rows, lanes))
            first = dot(tables, high)
            found.append(first[: 2 * KX] + first[2 * KX :] + dot(tables[: 2 * KX], low))
        turned[...] = jnp.concatenate(found, axis=0).T
        for t in range(quarter):
            pieces = [turned[pl.ds(4 * t + j, PACK, stride=KZ), :] for j in range(4)]
            for a, value in enumerate(regroup(pieces)):
                k, r = a // 2, a % 2
                spec[r, g * PACK : (g + 1) * PACK, (k * quarter + t) * 128 : (k * quarter + t + 1) * 128] = value

    def mix(tile, carry):
        here = pl.ds(pl.multiple_of(tile * 128, 128), 128)
        load(tile).wait()
        real = imag = None
        for i in range(channels):
            s_real, s_imag = spec[0, i : i + 1, here], spec[1, i : i + 1, here]
            w_real, w_imag = weights[tile, 0, i], weights[tile, 1, i]
            add_real = s_real * w_real - s_imag * w_imag
            add_imag = s_real * w_imag + s_imag * w_real
            real = add_real if real is None else real + add_real
            imag = add_imag if imag is None else imag + add_imag
        mixed[0, :, here] = real
        mixed[1, :, here] = imag
        return carry

    lax.fori_loop(0, weight_tiles, mix, 0)
    for g in range(groups):
        for t in range(quarter):
            pieces = [
                mixed[a % 2, g * PACK : (g + 1) * PACK, ((a // 2) * quarter + t) * 128 : ((a // 2) * quarter + t + 1) * 128]
                for a in range(4)
            ]
            for j, value in enumerate(regroup(pieces)):
                turned[pl.ds(4 * t + j, PACK, stride=KZ), :] = value
        modes = turned[...].T
        for k in range(local):
            high, low = split(modes[k * 2 * KX : (k + 1) * 2 * KX])
            spread = dot(back_table, jnp.concatenate([high, low, high], axis=0))
            spread = spread.reshape(devices, rows, lanes)
            at = (k * groups + g) * size
            for part, out_ref in enumerate(out_refs):
                out_ref[:, at : at + size, :] = spread[:, part * size : (part + 1) * size]


def middle(gathered, spectral_weight, length_x, local, groups, parts):
    channels = spectral_weight.shape[1]
    devices, height, lanes = gathered.shape
    ahead, back = middle_tables(length_x)
    modes = spectral_weight.shape[3]
    whole = pl.BlockSpec(memory_space=pltpu.VMEM)
    return pl.pallas_call(
        functools.partial(middle_body, local, groups, parts),
        out_shape=[jax.ShapeDtypeStruct((devices, height // parts, lanes), F32)] * parts,
        in_specs=[whole, pl.BlockSpec(memory_space=pltpu.HBM), whole, whole],
        out_specs=[whole] * parts,
        scratch_shapes=[
            pltpu.VMEM((PACK * KZ, local * 2 * KX), F32),
            pltpu.VMEM((2, channels, modes), F32),
            pltpu.VMEM((2, channels, modes), F32),
            pltpu.VMEM((modes // 128, 2, channels, channels, 128), F32),
            pltpu.SemaphoreType.DMA((modes // 128,)),
        ],
        compiler_params=pltpu.CompilerParams(vmem_limit_bytes=32 << 20),
        name="middle_x",
    )(
        gathered,
        pltpu.with_memory_space_constraint(spectral_weight, pltpu.HBM),
        jnp.asarray(ahead),
        jnp.asarray(back),
    )


def final_tables(length_x, length_y, length_z):
    y_phase = np_phase(np.arange(length_y), np_modes(KY), length_y)
    high, low = split_np(np.concatenate([np.cos(y_phase), np.sin(y_phase)], axis=1))
    ones = np.zeros((length_y, 16), np.float32)
    ones[:, :3] = 1.0
    y_table = np.concatenate([high, high, low, ones.astype(jnp.bfloat16)], axis=1)
    z_phase = np_phase(np.arange(length_z), np.arange(KZ), length_z).T
    factor = np.where(np.arange(KZ) == 0, 1.0, 2.0)[:, None] * (0.5 / (1.0 * length_x * length_y * length_z))
    z_high, z_low = split_np(np.concatenate([factor * np.cos(z_phase), -factor * np.sin(z_phase)], axis=0))
    z_table = np.zeros((2, 256, length_z), jnp.bfloat16)
    for slot in range(2):
        at = slot * 64
        z_table[slot, at : at + 32] = z_high
        z_table[slot, at + 32 : at + 64] = z_low
        z_table[slot, 128 + at : 128 + at + 32] = z_high
    lanes = PACK * KZ
    pick = np.zeros((2, lanes, 2, PACK, 2, 2, KZ), np.float32)
    kz = np.arange(KZ)
    for o in range(PACK):
        for copy in range(2):
            pick[0, o * KZ + kz, 0, o, copy, 0, kz] = 1.0
            pick[1, o * KZ + kz, 0, o, copy, 1, kz] = 1.0
            pick[1, o * KZ + kz, 1, o, copy, 0, kz] = -1.0
            pick[0, o * KZ + kz, 1, o, copy, 1, kz] = 1.0
    pick = pick.reshape(2 * lanes, PACK * lanes).astype(jnp.bfloat16)
    return lane_tiles(y_table), np.stack([lane_tiles(table) for table in z_table]), lane_tiles(pick)


def final_body(rows, first_plane, modes_ref, feat_ref, kron_ref, bias_ref, y_ref, z_ref, pick_ref, *rest):
    out_ref, picked, half, feats_in, results, arrivals, departures = rest[-7:]
    count, _, blocks = feats_in.shape[:3]
    span = blocks // PIECES

    def load(plane):
        return pltpu.make_async_copy(feat_ref.at[:, first_plane + plane], feats_in.at[plane], arrivals.at[plane])

    def leave(plane, piece):
        slot = plane % 2
        at = pl.ds(piece * span, span)
        return pltpu.make_async_copy(
            results.at[slot, :, at], out_ref.at[:, first_plane + plane, at], departures.at[slot, piece]
        )

    load(0).start()
    channels = feat_ref.shape[0]
    groups = channels // PACK
    length_y = y_ref.shape[1]
    length_z = feat_ref.shape[3] * 16
    lanes = PACK * KZ
    pairs = PACK // 2

    def prepare(plane):
        stacked = []
        for g in range(groups):
            row = g * rows + plane * 2
            real = modes_ref[pl.ds(row, KY, stride=groups * rows), :]
            imag = modes_ref[pl.ds(row + 1, KY, stride=groups * rows), :]
            high, low = split(jnp.concatenate([real, imag], axis=1))
            stacked += [high, low]
        left = jnp.concatenate(stacked, axis=0)
        for at in range(0, 2 * pairs, 2):
            value = dot(left, jnp.concatenate([pick_ref[at], pick_ref[at + 1]], axis=1)).astype(BF16)
            picked[at] = value[:, :lanes]
            picked[at + 1] = value[:, lanes:]
        y_table = wide(y_ref)[:, : 6 * KY + 16]
        for g in range(groups):
            high, low = 2 * g * KY, (2 * g + 1) * KY
            for f in range(pairs // 2):
                parts = [
                    jnp.concatenate(
                        [picked[s * pairs + 2 * f + t, h : h + KY, :] for h in (high, low, high) for s in range(2)]
                        + [bias_ref[g * pairs + 2 * f + t]],
                        axis=0,
                    )
                    for t in range(2)
                ]
                found = dot(y_table, jnp.concatenate(parts, axis=1))
                found = found.reshape(length_y // 8, 8, 2 * lanes)
                found = jnp.concatenate([found[:, :, :lanes], found[:, :, lanes:]], axis=1)
                top = found.astype(BF16)
                first = (g * pairs + 2 * f) * 8
                half[0, :, first : first + 16, :] = top
                half[1, :, first : first + 16, :] = (found - top.astype(F32)).astype(BF16)

    kron = wide(kron_ref)
    z_tables = [wide(z_ref.at[slot]) for slot in range(2)]
    size = channels * 4

    def one(plane, carry):
        slot = plane % 2

        @pl.when(plane >= 2)
        def drain():
            for piece in range(PIECES):
                leave(plane - 2, piece).wait()

        prepare(plane)
        load(plane).wait()

        @pl.when(plane == 0)
        def second():
            load(1).start()

        @pl.when(plane + 2 < count)
        def ahead():
            load(plane + 2).start()

        for b in range(blocks):
            feats = rows_of(feats_in[plane, :, b]).astype(BF16)
            left = jnp.concatenate([half[0, b], half[1, b]], axis=1)
            for side in range(2):
                h = dot(kron[side * size : (side + 1) * size], feats) + dot(left, z_tables[side])
                inner = h * (h * h * (8.0 * 0.7978845608 * 0.044715) + 2.0 * 0.7978845608)
                result = (h * jnp.tanh(inner) + h).reshape(channels // 2, 8, length_z)
                parts = [result[:, :, t * 128 : (t + 1) * 128] for t in range(length_z // 128)]
                result = jnp.concatenate(parts, axis=1).astype(BF16)
                for i in range(channels // 2):
                    results[slot, 2 * i + side, b] = result[i]
            if (b + 1) % span == 0:
                leave(plane, b // span).start()
        return carry

    lax.fori_loop(0, count, one, 0)
    for plane in range(max(count - 2, 0), count):
        for piece in range(PIECES):
            leave(plane, piece).wait()


def final_operands(features, pointwise_weight, pointwise_bias, length_x):
    length_y, length_z = features.shape[2:]
    lanes = PACK * KZ
    tables = [jnp.asarray(table) for table in final_tables(length_x, length_y, length_z)]
    channels = features.shape[0]
    weight = 0.5 * pointwise_weight.astype(F32)
    weight = weight.reshape(channels // 2, 2, channels).swapaxes(0, 1).reshape(channels, channels)
    kron = jnp.kron(weight, jnp.eye(8, dtype=F32)).astype(BF16)
    kron = kron.reshape(channels * 8, channels // 16, 128).swapaxes(0, 1)
    bias = pointwise_bias * (1.0 * length_x * length_y * length_z)
    b0 = lax.reduce_precision(bias, 8, 7)
    b1 = lax.reduce_precision(bias - b0, 8, 7)
    b2 = bias - b0 - b1
    pieces = jnp.stack([b0, b1, b2], axis=0).reshape(3, channels // 2, 2).swapaxes(0, 1).astype(BF16)
    pieces = jnp.pad(pieces[:, :, :, None, None], ((0, 0), (0, 13), (0, 0), (0, 0), (0, 31)))
    pieces = jnp.broadcast_to(pieces, (channels // 2, 16, 2, 2, 32)).reshape(channels // 2, 16, lanes)
    return [kron, pieces] + tables


def final(spread, tiles, operands, first_plane, count, before):
    channels, planes, blocks, height = tiles.shape[:4]
    rows = 2 * count
    groups = channels // PACK
    lanes = PACK * KZ
    whole = pl.BlockSpec(memory_space=pltpu.VMEM)
    apart = pl.BlockSpec(memory_space=pltpu.HBM)
    in_specs = [whole, apart] + [whole] * len(operands)
    arguments = [spread, tiles] + operands
    aliases = {}
    if before is not None:
        aliases = {len(arguments): 0}
        in_specs.append(apart)
        arguments.append(before)
    points = channels * count * blocks * 8 * height * 16
    return pl.pallas_call(
        functools.partial(final_body, rows, first_plane),
        out_shape=jax.ShapeDtypeStruct(tiles.shape, BF16),
        in_specs=in_specs,
        out_specs=apart,
        scratch_shapes=[
            pltpu.VMEM((PACK, groups * 2 * KY, lanes), BF16),
            pltpu.VMEM((2, blocks, channels * 4, lanes), BF16),
            pltpu.VMEM((count, channels, blocks, height, 128), BF16),
            pltpu.VMEM((2, channels, blocks, height, 128), BF16),
            pltpu.SemaphoreType.DMA((count,)),
            pltpu.SemaphoreType.DMA((2, PIECES)),
        ],
        input_output_aliases=aliases,
        cost_estimate=pl.CostEstimate(flops=points * 2000, bytes_accessed=4 * points, transcendentals=points),
        compiler_params=pltpu.CompilerParams(vmem_limit_bytes=40 << 20),
        name="final_yz",
    )(*arguments)


def exchange(values):
    arrived = []
    for value in values:
        if arrived:
            value, arrived[-1] = lax.optimization_barrier((value, arrived[-1]))
        arrived.append(lax.all_to_all(value, "px", split_axis=0, concat_axis=0))
    return arrived


def fused(devices, features, pointwise_weight, pointwise_bias, spectral_weight):
    channels, planes = features.shape[:2]
    length_x = planes * devices
    local = KY // devices
    groups = channels // PACK
    lanes = PACK * KZ
    count = planes // PARTS
    shape = (devices, local * groups * 2 * planes, lanes)
    tiles = tile_view(features)
    partial_value = forward(tiles, 0, planes, 4).reshape(shape)
    partial_value, pointwise_weight, pointwise_bias = lax.optimization_barrier(
        (partial_value, pointwise_weight, pointwise_bias)
    )
    operands = final_operands(features, pointwise_weight, pointwise_bias, length_x)
    gathered = lax.all_to_all(partial_value, "px", split_axis=0, concat_axis=0)
    gathered, operands[0], operands[1] = lax.optimization_barrier((gathered, operands[0], operands[1]))
    spreads = middle(gathered, spectral_weight, length_x, local, groups, PARTS)
    out = None
    for part, spread in enumerate(exchange(spreads)):
        spread = spread.reshape(KY * groups * 2 * count, lanes)
        out = final(spread, tiles, operands, part * count, count, out)
    return from_tile_view(out)


def signed_modes(number):
    ladder = jnp.arange(number, dtype=jnp.int32)
    return jnp.where(ladder < number // 2, ladder, ladder - number)


def phase_table(positions, frequency, length):
    product = positions[:, None] * frequency[None, :] % length
    return product.astype(jnp.float32) * (TWO_PI / length)


def forward_table(positions):
    x_phase = phase_table(positions, signed_modes(KX), positions.shape[0])
    cosine = jnp.cos(x_phase)
    sine = jnp.sin(x_phase)
    return jnp.stack(
        [jnp.stack([cosine, -sine], axis=1), jnp.stack([sine, cosine], axis=1)], axis=0
    )


def inverse_table(positions):
    x_phase = phase_table(positions, signed_modes(KX), positions.shape[0])
    cosine = jnp.cos(x_phase)
    sine = jnp.sin(x_phase)
    return jnp.stack(
        [jnp.stack([cosine, sine], axis=1), jnp.stack([-sine, cosine], axis=1)], axis=0
    )


def spectra_local(features):
    channels, planes, Y, Z = features.shape
    z_phase = phase_table(jnp.arange(Z, dtype=jnp.int32), jnp.arange(KZ, dtype=jnp.int32), Z)
    z_table = jnp.concatenate([jnp.cos(z_phase), -jnp.sin(z_phase)], axis=1).astype(jnp.bfloat16)
    flat = features.reshape(channels * planes * Y, Z)
    along_z = jnp.dot(flat, z_table, preferred_element_type=jnp.float32)
    stacked = along_z.reshape(channels, planes, Y, 2, KZ).transpose(3, 0, 1, 4, 2)
    y_phase = phase_table(jnp.arange(Y, dtype=jnp.int32), signed_modes(KY), Y)
    cosine = jnp.einsum(
        "rcxky,yj->rcxjk", stacked, jnp.cos(y_phase), precision=lax.Precision.HIGHEST
    )
    sine = jnp.einsum("rcxky,yj->rcxjk", stacked, jnp.sin(y_phase), precision=lax.Precision.HIGHEST)
    real_part = cosine[0] + sine[1]
    imag_part = cosine[1] - sine[0]
    return jnp.stack([real_part, imag_part]).reshape(2, channels, planes, KY * KZ)


def along_first(partial_value, table):
    return jnp.einsum("rcxq,rxsk->qsck", partial_value, table, precision=lax.Precision.HIGHEST)


def contract(left, right):
    return jnp.einsum("im,iom->om", left, right, precision=lax.Precision.HIGHEST)


def mix_modes(spectrum, weights):
    real_part = contract(spectrum[0], weights[0]) - contract(spectrum[1], weights[1])
    imag_part = contract(spectrum[0], weights[1]) + contract(spectrum[1], weights[0])
    return jnp.stack([real_part, imag_part])


def back_first(blended, table):
    return jnp.einsum("rcqk,rxsk->scxq", blended, table, precision=lax.Precision.HIGHEST)


def finish_planes(length_x, spread, features, pointwise_weight, pointwise_bias):
    channels, planes, Y, Z = features.shape
    X = length_x
    folded = spread.reshape(2, channels, planes, KY, KZ)
    y_phase = phase_table(jnp.arange(Y, dtype=jnp.int32), signed_modes(KY), Y)
    cosine = jnp.einsum(
        "rcxjk,yj->rcxky", folded, jnp.cos(y_phase), precision=lax.Precision.HIGHEST
    )
    sine = jnp.einsum("rcxjk,yj->rcxky", folded, jnp.sin(y_phase), precision=lax.Precision.HIGHEST)
    halves = jnp.concatenate([cosine[0] - sine[1], sine[0] + cosine[1]], axis=2)
    z_phase = phase_table(jnp.arange(Z, dtype=jnp.int32), jnp.arange(KZ, dtype=jnp.int32), Z)
    factor = jnp.where(jnp.arange(KZ, dtype=jnp.int32) == 0, 1.0, 2.0).astype(jnp.float32) / (
        1.0 * X * Y * Z
    )
    z_table = jnp.concatenate(
        [factor[:, None] * jnp.cos(z_phase).T, -factor[:, None] * jnp.sin(z_phase).T], axis=0
    )
    spectral = jnp.einsum("cxjy,jz->cxyz", halves, z_table, precision=lax.Precision.HIGHEST)
    linear = jnp.dot(
        pointwise_weight,
        features.reshape(channels, planes * Y * Z),
        preferred_element_type=jnp.float32,
    ).reshape(channels, planes, Y, Z)
    summed = spectral + linear + pointwise_bias[:, None, None, None]
    inner = 0.7978845608 * (summed + 0.044715 * summed * summed * summed)
    return (0.5 * summed * (1.0 + jnp.tanh(inner))).astype(jnp.bfloat16)


def plain(length_x, features, pointwise_weight, pointwise_bias, spectral_weight):
    every_plane = jnp.arange(length_x, dtype=jnp.int32)
    channels = features.shape[0]
    partial_value = spectra_local(features)
    gathered = lax.all_to_all(partial_value, "px", split_axis=3, concat_axis=2, tiled=True)
    spectrum = along_first(gathered, forward_table(every_plane)).transpose(1, 2, 0, 3)
    local_pairs = spectrum.shape[2]
    blended = mix_modes(
        spectrum.reshape(2, channels, local_pairs * KX), spectral_weight
    ).reshape(
        2, channels, local_pairs, KX
    )
    spread = lax.all_to_all(
        back_first(blended, inverse_table(every_plane)),
        "px",
        split_axis=2,
        concat_axis=3,
        tiled=True,
    )
    return finish_planes(length_x, spread, features, pointwise_weight, pointwise_bias)


def on_device(devices, features, pointwise_weight, pointwise_bias, spectral_weight):
    channels, planes, length_y, length_z = features.shape
    fits = (
        KY == 2 * devices
        and planes % 8 == 0
        and channels == 32
        and planes * length_y * length_z <= 1 << 19
        and length_y % 128 == 0
        and length_z == 256
    )
    call = functools.partial(fused, devices) if fits else functools.partial(plain, planes * devices)
    return call(features, pointwise_weight, pointwise_bias, spectral_weight)


def solution(mesh):
    in_specs = (P(None, ("groups", "px"), None, None), P(), P(), P(None, None, None, "px"))
    out_specs = P(None, ("groups", "px"), None, None)
    return jax.shard_map(
        functools.partial(on_device, mesh.shape["px"]),
        mesh=mesh,
        in_specs=in_specs,
        out_specs=out_specs,
        check_vma=False,
    )
```
